16 devices in a mesh: dp: 2 (over z), emb: 8 (over y, x, core).
Axes of the slice: x: 2, y: 2, z: 2, core: 2. Of those that a mesh axis runs over, the one named last changes fastest.
Arguments:
- token_ids: int32 [65536], P(('dp', 'emb'))
- x_init: bfloat16 [65536, 768], P(('dp', 'emb'))
- d_out: bfloat16 [65536, 768], P(('dp', 'emb'))
- tables: bfloat16 [4, 50304, 768], P(None, 'emb')
- w_up: bfloat16 [4, 768, 3072], replicated
- w_down: bfloat16 [4, 3072, 768], replicated
- w_gate: bfloat16 [4, 768, 768], replicated
- w_proj: bfloat16 [4, 768, 768], replicated
Outputs:
- output 1: bfloat16 [65536, 768], P(('dp', 'emb'))
- output 2: float32 [4, 50304, 768], P(None, 'emb')
All inputs are finite; a program needn't handle non-finite values.
Results may differ from the reference program's by a relative error of at most 0.0111161.
Values are sent between devices in bfloat16 or wider.
A program may use at most 1 GiB of HBM per device.

```python
import jax
import jax.numpy as jnp
from jax import lax

MODEL_DIM = 768
FF_DIM = 3072
EMB_DIM = 768
VOCAB_SIZE = 50304
LAYERS = 4
TOK_DEV = 4096
DP_SIZE = 2
EMB_SIZE = 8

NORM_EPS = 1e-6
DEVICES = DP_SIZE * EMB_SIZE
TOKENS = TOK_DEV * DEVICES
ROWS_DEV = VOCAB_SIZE // EMB_SIZE


def draw_ids(rng_key):
    k_shift, k_perm, k_order, k_coin, k_hot, k_span, k_wide = jax.random.split(rng_key, 7)
    half_emb = EMB_SIZE // 2
    mean_count = TOK_DEV // EMB_SIZE
    shifts = jax.random.randint(k_shift, (DEVICES, half_emb), 0, mean_count + 1)
    shifts = shifts.at[0, 0].set(mean_count)
    pair_counts = jnp.stack([mean_count + shifts, mean_count - shifts], axis=2).reshape(DEVICES, EMB_SIZE)
    owner_perm = jax.vmap(lambda sub_key: jax.random.permutation(sub_key, EMB_SIZE))(jax.random.split(k_perm, DEVICES))
    bounds = jnp.cumsum(pair_counts, axis=1)
    positions = jnp.arange(TOK_DEV, dtype=jnp.int32)
    which_pos = jnp.sum((positions[None, :, None] >= bounds[:, None, :]).astype(jnp.int32), axis=2)
    owners = jnp.take_along_axis(owner_perm, which_pos, axis=1)
    owners = jax.vmap(lambda sub_key, own_row: jax.random.permutation(sub_key, own_row))(jax.random.split(k_order, DEVICES), owners)
    coin_flip = jax.random.randint(k_coin, (DEVICES, TOK_DEV), 0, 2)
    hot_off = jax.random.randint(k_hot, (DEVICES, TOK_DEV), 0, 64)
    span_top = jax.random.randint(k_span, (DEVICES, TOK_DEV), 1, ROWS_DEV + 1)
    wide_off = jax.random.randint(k_wide, (DEVICES, TOK_DEV), 0, span_top)
    offsets = jnp.where(coin_flip == 1, hot_off, wide_off)
    return (owners * ROWS_DEV + offsets).reshape(TOKENS).astype(jnp.int32)


def setup_inputs(seed: int = 0) -> dict:
    rng_key = jax.random.key(seed)
    k_ids, k_x, k_dy, k_tab, k_up, k_down, k_gate, k_proj = jax.random.split(rng_key, 8)
    return {
        'token_ids': draw_ids(k_ids),
        'x_init': jax.random.normal(k_x, (TOKENS, MODEL_DIM), jnp.float32).astype(jnp.bfloat16),
        'd_out': jax.random.normal(k_dy, (TOKENS, MODEL_DIM), jnp.float32).astype(jnp.bfloat16),
        'tables': jax.random.normal(k_tab, (LAYERS, VOCAB_SIZE, EMB_DIM), jnp.float32).astype(jnp.bfloat16),
        'w_up': (jax.random.normal(k_up, (LAYERS, MODEL_DIM, FF_DIM), jnp.float32) * MODEL_DIM ** -0.5).astype(jnp.bfloat16),
        'w_down': (jax.random.normal(k_down, (LAYERS, FF_DIM, MODEL_DIM), jnp.float32) * (0.5 * FF_DIM ** -0.5)).astype(jnp.bfloat16),
        'w_gate': (jax.random.normal(k_gate, (LAYERS, MODEL_DIM, EMB_DIM), jnp.float32) * MODEL_DIM ** -0.5).astype(jnp.bfloat16),
        'w_proj': (jax.random.normal(k_proj, (LAYERS, EMB_DIM, MODEL_DIM), jnp.float32) * (0.4 * EMB_DIM ** -0.5)).astype(jnp.bfloat16),
    }


def rms_scale(x_f32):
    return lax.rsqrt(jnp.mean(x_f32 * x_f32, axis=-1, keepdims=True) + NORM_EPS)


def gelu_back(pre_act, grad_out):
    _, pull_back = jax.vjp(jax.nn.gelu, pre_act)
    return pull_back(grad_out)[0]


def block_pass(tok_ids, x_blk, dy_blk, tables, w_up, w_down, w_gate, w_proj):
    def fwd_step(x_in, layer_args):
        layer_tab, up_w, down_w, gate_w, proj_w = layer_args
        x_f32 = x_in.astype(jnp.float32)
        normed = (x_f32 * rms_scale(x_f32)).astype(jnp.bfloat16)
        hidden = jax.nn.gelu(jnp.dot(normed, up_w, preferred_element_type=jnp.float32)).astype(jnp.bfloat16)
        gate_val = jax.nn.gelu(jnp.dot(normed, gate_w, preferred_element_type=jnp.float32)).astype(jnp.bfloat16)
        emb_rows = jnp.take(layer_tab, tok_ids, axis=0)
        mixed_rows = (gate_val.astype(jnp.float32) * emb_rows.astype(jnp.float32)).astype(jnp.bfloat16)
        new_x = x_f32 + jnp.dot(hidden, down_w, preferred_element_type=jnp.float32) + jnp.dot(mixed_rows, proj_w, preferred_element_type=jnp.float32)
        return new_x.astype(jnp.bfloat16), (x_in, emb_rows)

    x_last, (x_saved, rows_saved) = lax.scan(fwd_step, x_blk, (tables, w_up, w_down, w_gate, w_proj))

    def bwd_step(d_next, layer_args):
        x_in, emb_rows, up_w, down_w, gate_w, proj_w = layer_args
        x_f32 = x_in.astype(jnp.float32)
        row_scale = rms_scale(x_f32)
        normed = x_f32 * row_scale
        norm_bf = normed.astype(jnp.bfloat16)
        pre_up = jnp.dot(norm_bf, up_w, preferred_element_type=jnp.float32)
        pre_gate = jnp.dot(norm_bf, gate_w, preferred_element_type=jnp.float32)
        gate_val = jax.nn.gelu(pre_gate).astype(jnp.bfloat16)
        d_mixed = jnp.dot(d_next, proj_w.T, preferred_element_type=jnp.float32).astype(jnp.bfloat16)
        grad_rows = gate_val.astype(jnp.float32) * d_mixed.astype(jnp.float32)
        d_emb = (d_mixed.astype(jnp.float32) * emb_rows.astype(jnp.float32)).astype(jnp.bfloat16)
        d_gate = gelu_back(pre_gate, d_emb.astype(jnp.float32)).astype(jnp.bfloat16)
        d_hidden = jnp.dot(d_next, down_w.T, preferred_element_type=jnp.float32).astype(jnp.bfloat16)
        d_up = gelu_back(pre_up, d_hidden.astype(jnp.float32)).astype(jnp.bfloat16)
        d_normed = jnp.dot(d_up, up_w.T, preferred_element_type=jnp.float32) + jnp.dot(d_gate, gate_w.T, preferred_element_type=jnp.float32)
        d_resid = row_scale * (d_normed - normed * jnp.mean(d_normed * normed, axis=-1, keepdims=True))
        return (d_next.astype(jnp.float32) + d_resid).astype(jnp.bfloat16), grad_rows

    _, grad_rows = lax.scan(bwd_step, dy_blk, (x_saved, rows_saved, w_up, w_down, w_gate, w_proj), reverse=True)
    return x_last, grad_rows


def reference(token_ids, x_init, d_out, tables, w_up, w_down, w_gate, w_proj):
    def one_block(blk_args):
        return block_pass(blk_args[0], blk_args[1], blk_args[2], tables, w_up, w_down, w_gate, w_proj)

    x_last, grad_rows = lax.map(one_block, (token_ids.reshape(DEVICES, TOK_DEV), x_init.reshape(DEVICES, TOK_DEV, MODEL_DIM), d_out.reshape(DEVICES, TOK_DEV, MODEL_DIM)))
    grad_rows = jnp.swapaxes(grad_rows, 0, 1).reshape(LAYERS, TOKENS, EMB_DIM)
    d_tables = jax.vmap(lambda layer_rows: jax.ops.segment_sum(layer_rows, token_ids, num_segments=VOCAB_SIZE))(grad_rows)
    return x_last.reshape(TOKENS, MODEL_DIM), d_tables
```

```python
import functools

import jax
import jax.numpy as jnp
from jax import lax
from jax.experimental import pallas as pl
from jax.experimental.pallas import tpu as pltpu
from jax.sharding import PartitionSpec as P

NORM_EPS = 1e-6
GELU_K = 0.7978845608028654
GELU_C = 0.044715
DEAD = 1 << 30
TILE = 512
HALF = 256
LAG = 1
SEG_TILE = 256
ROWS = 256
CHUNKS = 4
VMEM = 66_000_000
BF = jnp.bfloat16
F32 = jnp.float32


def dot(a, b):
    return lax.dot_general(a, b, (((1,), (0,)), ((), ())), preferred_element_type=F32)


def dot_t(a, b):
    return lax.dot_general(a, b, (((1,), (1,)), ((), ())), preferred_element_type=F32)


def gelu_both(p):
    sq = p * p
    half = 0.5 * jnp.tanh(p * (GELU_K + (GELU_K * GELU_C) * sq))
    cdf = 0.5 + half
    value = p * cdf
    slope = (0.5 - half) * (2.0 * GELU_K + (6.0 * GELU_K * GELU_C) * sq)
    return value, cdf + value * slope


def weave(streams):
    waiting = [LAG * k for k in range(len(streams))]
    alive = list(streams)
    while alive:
        for k, stream in enumerate(streams):
            if stream not in alive:
                continue
            if waiting[k] > 0:
                waiting[k] -= 1
            elif next(stream, None) is None:
                alive.remove(stream)


def forward_kernel(last, nt_ref, x_ref, e_ref, wu_ref, wd_ref, wg_ref, wp_ref, *rest):
    pl.when(pl.program_id(1) < nt_ref[0])(lambda: forward_tile(last, x_ref, e_ref, wu_ref, wd_ref, wg_ref, wp_ref, *rest))


def forward_tile(last, x_ref, e_ref, wu_ref, wd_ref, wg_ref, wp_ref, *rest):
    if last:
        xl_ref, du_ref, dg_ref, a_ref, out_ref, x_scr, sem = rest
    else:
        xl_ref, du_ref, dg_ref, a_ref, x_scr, sem = rest
    layer, tile = pl.program_id(0), pl.program_id(1)
    size = xl_ref.shape[1]

    @pl.when(jnp.logical_and(layer == 0, tile == 0))
    def _():
        copy = pltpu.make_async_copy(x_ref, x_scr, sem)
        copy.start()
        copy.wait()

    ff = wu_ref.shape[2]
    step = ff // CHUNKS
    cols = [slice(c * step, (c + 1) * step) for c in range(CHUNKS)]

    def stream(k, down):
        part = slice(k * HALF, (k + 1) * HALF)
        rows = pl.ds(pl.multiple_of(tile * size + k * HALF, HALF), HALF)
        x_bf = x_scr[rows, :]
        xl_ref[0, part, :] = x_bf
        x = x_bf.astype(F32)
        r = lax.rsqrt(jnp.mean(x * x, axis=-1, keepdims=True) + NORM_EPS)
        u = (x * r).astype(BF)
        pre_gate = dot(u, wg_ref[0])
        now = dot(u, wu_ref[0, :, cols[0]])
        yield True
        gate, d_gate = gelu_both(pre_gate)
        a = gate.astype(BF)
        a_ref[0, part, :] = a
        dg_ref[0, part, :] = d_gate
        acc = None
        for c in range(CHUNKS):
            if c + 1 < CHUNKS:
                later = dot(u, wu_ref[0, :, cols[c + 1]])
            h, d_up = gelu_both(now)
            du_ref[0, part, cols[c]] = d_up
            if down:
                if c == 0:
                    s = (a.astype(F32) * e_ref[0, part, :].astype(F32)).astype(BF)
                    acc = x + dot(s, wp_ref[0])
                acc = acc + dot(h.astype(BF), wd_ref[0, cols[c], :])
            if c + 1 < CHUNKS:
                now = later
            yield True
        if down:
            x_new = acc.astype(BF)
            x_scr[rows, :] = x_new
            if last:
                out_ref[part, :] = x_new

    def run(down):
        weave([stream(k, down) for k in range(size // HALF)])

    if last:
        run(True)
    else:
        is_last = layer == pl.num_programs(0) - 1
        pl.when(jnp.logical_not(is_last))(lambda: run(True))
        pl.when(is_last)(lambda: run(False))


def backward_kernel(nt_ref, n_ref, *refs):
    pl.when(pl.program_id(1) < nt_ref[0])(lambda: backward_tile(n_ref, *refs))


def backward_tile(n_ref, d_ref, xl_ref, du_ref, dg_ref, a_ref, e_ref, wu_ref, wd_ref, wg_ref, wp_ref, hi_ref, lo_ref, c_scr, sem):
    step_id, tile = pl.program_id(0), pl.program_id(1)
    size = xl_ref.shape[1]

    @pl.when(jnp.logical_and(step_id == 0, tile == 0))
    def _():
        copy = pltpu.make_async_copy(d_ref, c_scr, sem)
        copy.start()
        copy.wait()

    ff = wu_ref.shape[2]
    step = ff // CHUNKS
    cols = [slice(c * step, (c + 1) * step) for c in range(CHUNKS)]

    def stream(k, down):
        part = slice(k * HALF, (k + 1) * HALF)
        rows = pl.ds(pl.multiple_of(tile * size + k * HALF, HALF), HALF)
        c = c_scr[rows, :]
        ds = dot_t(c, wp_ref[0]).astype(BF)
        if down:
            now = dot_t(c, wd_ref[0, cols[0], :])
            later = dot_t(c, wd_ref[0, cols[1], :])
        yield True
        ds_f = ds.astype(F32)
        live = tile * size + k * HALF + lax.broadcasted_iota(jnp.int32, ds_f.shape, 0) < n_ref[0]
        grad = jnp.where(live, a_ref[0, part, :].astype(F32) * ds_f, 0.0)
        hi = grad.astype(BF)
        hi_ref[0, part, :] = hi
        lo_ref[0, part, :] = (grad - hi.astype(F32)).astype(BF)
        if down:
            de = (ds_f * e_ref[0, part, :].astype(F32)).astype(BF)
            dgate = (dg_ref[0, part, :] * de.astype(F32)).astype(BF)
            yield True
            m = dot_t(dgate, wg_ref[0])
            for q in range(CHUNKS):
                dup = (du_ref[0, part, cols[q]] * now.astype(BF).astype(F32)).astype(BF)
                now = later
                if q + 2 < CHUNKS:
                    later = dot_t(c, wd_ref[0, cols[q + 2], :])
                m = m + dot_t(dup, wu_ref[0, :, cols[q]])
                yield True
            x = xl_ref[0, part, :].astype(F32)
            r = lax.rsqrt(jnp.mean(x * x, axis=-1, keepdims=True) + NORM_EPS)
            n = x * r
            corr = jnp.mean(m * n, axis=-1, keepdims=True)
            c_scr[rows, :] = (c.astype(F32) + r * (m - n * corr)).astype(BF)

    def run(down):
        weave([stream(k, down) for k in range(size // HALF)])

    bottom = step_id == pl.num_programs(0) - 1
    pl.when(jnp.logical_not(bottom))(lambda: run(True))
    pl.when(bottom)(lambda: run(False))


def run_forward(last, nt, x, e, w_up, w_down, w_gate, w_proj):
    n, dim = x.shape
    layers, _, ff = w_up.shape
    t = TILE

    def per_layer(l, i, nt_ref):
        return (l, 0, 0)

    def saved(l, i, nt_ref):
        return (jnp.maximum(l - 1, 0), jnp.minimum(i, nt_ref[0] - 1), 0)

    def tok(l, i, nt_ref):
        return (l, jnp.minimum(i, nt_ref[0] - 1), 0)

    outs = [
        (jax.ShapeDtypeStruct((layers - 1, n, dim), BF), pl.BlockSpec((1, t, dim), saved)),
        (jax.ShapeDtypeStruct((layers - 1, n, ff), F32), pl.BlockSpec((1, t, ff), saved)),
        (jax.ShapeDtypeStruct((layers - 1, n, dim), F32), pl.BlockSpec((1, t, dim), saved)),
        (jax.ShapeDtypeStruct((layers, n, dim), BF), pl.BlockSpec((1, t, dim), tok)),
    ]
    if last:
        outs.append((jax.ShapeDtypeStruct((n, dim), BF), pl.BlockSpec((t, dim), lambda l, i, nt_ref: (jnp.minimum(i, nt_ref[0] - 1), 0))))
    flops = layers * n * 2 * dim * (2 * ff + 2 * dim)
    return pl.pallas_call(
        functools.partial(forward_kernel, last),
        out_shape=[o[0] for o in outs],
        grid_spec=pltpu.PrefetchScalarGridSpec(
            num_scalar_prefetch=1, grid=(layers, n // t),
            in_specs=[pl.BlockSpec(memory_space=pl.ANY), pl.BlockSpec((1, t, dim), tok),
                      pl.BlockSpec((1, dim, ff), per_layer), pl.BlockSpec((1, ff, dim), per_layer),
                      pl.BlockSpec((1, dim, dim), per_layer), pl.BlockSpec((1, dim, dim), per_layer)],
            out_specs=[o[1] for o in outs],
            scratch_shapes=[pltpu.VMEM((n, dim), BF), pltpu.SemaphoreType.DMA]),
        compiler_params=pltpu.CompilerParams(dimension_semantics=("arbitrary", "arbitrary"), vmem_limit_bytes=VMEM),
        cost_estimate=pl.CostEstimate(flops=flops // 2, bytes_accessed=n * ff * 4 * layers, transcendentals=0),
        name="fwd",
    )(nt, x, e, w_up, w_down, w_gate, w_proj)


def run_backward(nt, n_live, d, xl, du, dg, a, e, w_up, w_down, w_gate, w_proj):
    n, dim = d.shape
    layers, _, ff = w_up.shape
    t = TILE
    top = layers - 1

    def per_layer(g, i, nt_ref, n_ref):
        return (top - g, 0, 0)

    def upper_layer(g, i, nt_ref, n_ref):
        return (jnp.maximum(top - g, 1), 0, 0)

    def saved(g, i, nt_ref, n_ref):
        return (jnp.maximum(top - 1 - g, 0), jnp.where(g == top, nt_ref[0] - 1, jnp.minimum(i, nt_ref[0] - 1)), 0)

    def tok(g, i, nt_ref, n_ref):
        return (top - g, jnp.minimum(i, nt_ref[0] - 1), 0)

    flops = layers * n * 2 * dim * (2 * ff + 2 * dim)
    return pl.pallas_call(
        backward_kernel,
        out_shape=[jax.ShapeDtypeStruct((layers, n, dim), BF)] * 2,
        grid_spec=pltpu.PrefetchScalarGridSpec(
            num_scalar_prefetch=2, grid=(layers, n // t),
            in_specs=[pl.BlockSpec(memory_space=pl.ANY), pl.BlockSpec((1, t, dim), saved),
                      pl.BlockSpec((1, t, ff), saved), pl.BlockSpec((1, t, dim), saved),
                      pl.BlockSpec((1, t, dim), tok), pl.BlockSpec((1, t, dim), tok),
                      pl.BlockSpec((1, dim, ff), upper_layer), pl.BlockSpec((1, ff, dim), upper_layer),
                      pl.BlockSpec((1, dim, dim), upper_layer), pl.BlockSpec((1, dim, dim), per_layer)],
            out_specs=[pl.BlockSpec((1, t, dim), tok)] * 2,
            scratch_shapes=[pltpu.VMEM((n, dim), BF), pltpu.SemaphoreType.DMA]),
        compiler_params=pltpu.CompilerParams(dimension_semantics=("arbitrary", "arbitrary"), vmem_limit_bytes=VMEM),
        cost_estimate=pl.CostEstimate(flops=flops // 2, bytes_accessed=n * ff * 4 * layers, transcendentals=0),
        name="bwd",
    )(nt, n_live, d, xl, du, dg, a, e, w_up, w_down, w_gate, w_proj)


def pick_kernel(rows_dev, num_ref, *refs):
    pl.when(pl.program_id(0) < num_ref[0])(lambda: pick_step(rows_dev, *refs))


def pick_step(rows_dev, tile_ref, blk_ref, off_ref, tab_ref, e_ref):
    p = pl.program_id(0)
    blk = blk_ref[p]
    layers, size = tab_ref.shape[0], tab_ref.shape[1]
    hot = (off_ref[0] - blk * size == lax.broadcasted_iota(jnp.int32, (size, off_ref.shape[2]), 0)).astype(F32)
    hot = hot.T.astype(BF)
    fresh = jnp.logical_or(p == 0, tile_ref[p] != tile_ref[jnp.maximum(p - 1, 0)])
    valid = rows_dev - blk * size
    tail = valid < size

    @pl.when(fresh)
    def _():
        e_ref[...] = jnp.zeros_like(e_ref)

    def work(clip):
        for l in range(layers):
            rows = tab_ref[l]
            if clip:
                keep = lax.broadcasted_iota(jnp.int32, rows.shape, 0) < valid
                rows = jnp.where(keep, rows.astype(F32), 0.0).astype(BF)
            e_ref[l] += dot(hot, rows).astype(BF)

    pl.when(tail)(lambda: work(True))
    pl.when(jnp.logical_not(tail))(lambda: work(False))


def run_pick(pairs, tile, blk, off, tables):
    layers, rows_dev, dim = tables.shape
    n = off.shape[0]
    t = SEG_TILE
    return pl.pallas_call(
        functools.partial(pick_kernel, rows_dev),
        out_shape=jax.ShapeDtypeStruct((layers, n, dim), BF),
        grid_spec=pltpu.PrefetchScalarGridSpec(
            num_scalar_prefetch=3, grid=(tile.shape[0],),
            in_specs=[pl.BlockSpec((1, 1, t), lambda p, nr, tr, br: (tr[p], 0, 0)),
                      pl.BlockSpec((layers, ROWS, dim), lambda p, nr, tr, br: (0, br[p], 0))],
            out_specs=pl.BlockSpec((layers, t, dim), lambda p, nr, tr, br: (0, tr[p], 0))),
        compiler_params=pltpu.CompilerParams(dimension_semantics=("arbitrary",), vmem_limit_bytes=VMEM),
        cost_estimate=pl.CostEstimate(flops=40_000_000_000, bytes_accessed=n * dim * 16, transcendentals=0),
        name="pick",
    )(pairs.reshape(1), tile, blk, off.reshape(n // t, 1, t), tables)


def sum_kernel(num_ref, *refs):
    pl.when(pl.program_id(0) < num_ref[0])(lambda: sum_step(*refs))


def sum_step(blk_ref, own_ref, dup_ref, sel_ref, pos_own, pos_dup, off_o, hi_o, lo_o, off_d, hi_d, lo_d, out_ref):
    s = pl.program_id(0)
    blk = blk_ref[s]
    layers, rows, dim = out_ref.shape
    t = off_o.shape[2]
    half = 128

    @pl.when(jnp.logical_or(s == 0, blk != blk_ref[jnp.maximum(s - 1, 0)]))
    def _():
        out_ref[...] = jnp.zeros_like(out_ref)

    def add(tile, pos, off_ref, hi_ref, lo_ref):
        first, end = pos[blk], pos[blk + 1]
        for j in range(t // half):
            at = tile * t + j * half

            @pl.when(jnp.logical_and(at < end, at + half > first))
            def _():
                cols = pl.ds(j * half, half)
                hot = (off_ref[0, :, cols] - blk * rows == lax.broadcasted_iota(jnp.int32, (rows, half), 0)).astype(F32).astype(BF)
                hot = jnp.concatenate([hot, hot], axis=1)
                for l in range(layers):
                    both = jnp.concatenate([hi_ref[l, cols, :], lo_ref[l, cols, :]], axis=0)
                    out_ref[l] += dot(hot, both)

    @pl.when(sel_ref[s] == 0)
    def _():
        add(own_ref[s], pos_own, off_o, hi_o, lo_o)

    @pl.when(sel_ref[s] == 1)
    def _():
        add(dup_ref[s], pos_dup, off_d, hi_d, lo_d)


def run_sum(rows_dev, steps, lists, off_own, hi_own, lo_own, off_dup, hi_dup, lo_dup):
    layers, n, dim = hi_own.shape
    t = SEG_TILE
    own = lambda s, m, b, o, d, se, po, pd: (0, o[s], 0)
    dup = lambda s, m, b, o, d, se, po, pd: (0, d[s], 0)
    own_off = lambda s, m, b, o, d, se, po, pd: (o[s], 0, 0)
    dup_off = lambda s, m, b, o, d, se, po, pd: (d[s], 0, 0)
    big = (layers, t, dim)
    return pl.pallas_call(
        sum_kernel,
        out_shape=jax.ShapeDtypeStruct((layers, rows_dev, dim), F32),
        grid_spec=pltpu.PrefetchScalarGridSpec(
            num_scalar_prefetch=7, grid=(lists[0].shape[0],),
            in_specs=[pl.BlockSpec((1, 1, t), own_off), pl.BlockSpec(big, own), pl.BlockSpec(big, own),
                      pl.BlockSpec((1, 1, t), dup_off), pl.BlockSpec(big, dup), pl.BlockSpec(big, dup)],
            out_specs=pl.BlockSpec((layers, ROWS, dim), lambda s, m, b, o, d, se, po, pd: (0, b[s], 0))),
        compiler_params=pltpu.CompilerParams(dimension_semantics=("arbitrary",), vmem_limit_bytes=VMEM),
        cost_estimate=pl.CostEstimate(flops=60_000_000_000, bytes_accessed=layers * dim * 4 * (2 * n + rows_dev), transcendentals=0),
        name="tabsum",
    )(steps.reshape(1), *lists, off_own.reshape(n // t, 1, t), hi_own, lo_own, off_dup.reshape(n // t, 1, t), hi_dup, lo_dup)


def spans(off, n_blocks):
    edges = jnp.arange(n_blocks + 1, dtype=jnp.int32) * ROWS
    pos = jnp.sum((off[None, :] < edges[:, None]).astype(jnp.int32), axis=1)
    first = pos[:-1] // SEG_TILE
    count = jnp.where(pos[1:] > pos[:-1], (pos[1:] - 1) // SEG_TILE - first + 1, 0)
    return pos, first, count


def pick_at(one_hot, values):
    return jnp.sum(one_hot * values[None, :], axis=1)


def expand(count, length):
    end = jnp.cumsum(count)
    step = jnp.minimum(jnp.arange(length, dtype=jnp.int32), end[-1] - 1)
    begin = end - count
    in_block = jnp.logical_and(step[:, None] >= begin[None, :], step[:, None] < end[None, :]).astype(jnp.int32)
    return in_block, step - pick_at(in_block, begin), end[-1]


def take_rows(rows, idx):
    return rows.at[idx].get(mode='promise_in_bounds')


def solution(mesh):
    emb_size = mesh.shape['emb']
    dp_size = mesh.shape['dp']
    tok_spec = P(('dp', 'emb'))
    row_spec = P(('dp', 'emb'), None)
    tab_spec = P(None, 'emb', None)
    full_spec = P()

    def device_body(ids, x_loc, dy_loc, tabs, w_up, w_down, w_gate, w_proj):
        tok_dev = ids.shape[0]
        layers, rows_dev, dim = tabs.shape
        cap = 2 * tok_dev // emb_size
        n = emb_size * cap
        n_blocks = -(-rows_dev // ROWS)
        iota_tok = jnp.arange(tok_dev, dtype=jnp.int32)
        iota_n = jnp.arange(n, dtype=jnp.int32)

        ids_sorted, order = lax.sort((ids, iota_tok), num_keys=1)
        bounds = jnp.arange(emb_size + 1, dtype=jnp.int32) * rows_dev
        starts = jnp.sum((ids[None, :] < bounds[:, None]).astype(jnp.int32), axis=1)
        ids_pad = jnp.concatenate([ids_sorted, jnp.full((cap,), DEAD, jnp.int32)])
        order_pad = jnp.concatenate([order, jnp.zeros((cap,), jnp.int32)])
        slot_id = jnp.stack([lax.dynamic_slice(ids_pad, (starts[o],), (cap,)) for o in range(emb_size)])
        slot_src = jnp.concatenate([lax.dynamic_slice(order_pad, (starts[o],), (cap,)) for o in range(emb_size)])
        rank = jnp.arange(cap, dtype=jnp.int32)[None, :]
        alive = rank < (starts[1:] - starts[:-1])[:, None]
        send_off = jnp.where(alive, slot_id - bounds[:-1, None], DEAD)
        recv_off = lax.all_to_all(send_off, 'emb', 0, 0, tiled=True).reshape(n)

        def exchange(rows):
            return lax.all_to_all(rows.reshape(emb_size, cap, dim), 'emb', 0, 0, tiled=True).reshape(n, dim)

        off_own, order_own = lax.sort((recv_off, iota_n), num_keys=1)
        swap = [(i, dp_size - 1 - i) for i in range(dp_size)]
        off_dup = lax.ppermute(off_own, 'dp', swap)

        def lookup(off):
            live = jnp.sum((off < DEAD).astype(jnp.int32)).reshape(1)
            tiles = jnp.maximum((live + TILE - 1) // TILE, 1)
            pos, first, count = spans(off, n_blocks)
            hot, inner, pairs = expand(count, n // SEG_TILE + n_blocks)
            tile = pick_at(hot, first) + inner
            blk = pick_at(hot, jnp.arange(n_blocks, dtype=jnp.int32))
            used = (live[0] + SEG_TILE - 1) // SEG_TILE
            extra = tiles[0] * (TILE // SEG_TILE) - used
            past = jnp.minimum(jnp.arange(tile.shape[0], dtype=jnp.int32) - pairs, extra - 1)
            tile = jnp.where(past < 0, tile, used + past)
            tile = jnp.clip(tile, 0, n // SEG_TILE - 1)
            return run_pick(pairs + extra, tile, blk, off, tabs), live, tiles, (pos, first, count)

        x_recv = exchange(take_rows(x_loc, slot_src))
        d_send = take_rows(dy_loc, slot_src)
        e_own, live_own, tiles_own, (pos_o, first_o, count_o) = lookup(off_own)
        e_dup, live_dup, tiles_dup, (pos_d, first_d, count_d) = lookup(off_dup)
        d_send, e_own, e_dup = lax.optimization_barrier((d_send, e_own, e_dup))
        x_recv, e_own, e_dup = lax.optimization_barrier((x_recv, e_own, e_dup))
        d_recv = exchange(d_send)
        x_own = take_rows(x_recv, order_own)
        d_own = take_rows(d_recv, order_own)
        x_dup = lax.ppermute(x_own, 'dp', swap)
        d_dup = lax.ppermute(d_own, 'dp', swap)
        weights = (w_up, w_down, w_gate, w_proj)

        def batch(last, e, live, tiles, x, d):
            xl, du, dg, a, *fin = run_forward(last, tiles, x, e, *weights)
            return *run_backward(tiles, live, d, xl, du, dg, a, e, *weights), *fin

        hi_own, lo_own, x_fin = batch(True, e_own, live_own, tiles_own, x_own, d_own)
        x_dup, hi_own, lo_own = lax.optimization_barrier((x_dup, hi_own, lo_own))
        hi_dup, lo_dup = batch(False, e_dup, live_dup, tiles_dup, x_dup, d_dup)

        _, back = lax.sort((order_own, iota_n), num_keys=1)
        _, place = lax.sort((order, iota_tok), num_keys=1)
        x_fin, hi_dup, lo_dup = lax.optimization_barrier((x_fin, hi_dup, lo_dup))
        returned = exchange(take_rows(x_fin, back))
        owner_hot = (ids[:, None] // rows_dev == jnp.arange(emb_size, dtype=jnp.int32)[None, :]).astype(jnp.int32)
        slot = place + pick_at(owner_hot, jnp.arange(emb_size, dtype=jnp.int32) * cap - starts[:-1])

        per_block = jnp.maximum(count_o + count_d, 1)
        hot, inner, steps = expand(per_block, 2 * (n // SEG_TILE + n_blocks))
        n_own = pick_at(hot, count_o)
        sel = (inner >= n_own).astype(jnp.int32)
        top = n // SEG_TILE - 1
        t_own = jnp.clip(pick_at(hot, first_o) + jnp.minimum(inner, jnp.maximum(n_own - 1, 0)), 0, top)
        t_dup = jnp.clip(pick_at(hot, first_d) + jnp.maximum(inner - n_own, 0), 0, top)
        blk = pick_at(hot, jnp.arange(n_blocks, dtype=jnp.int32))
        d_tabs = run_sum(rows_dev, steps, (blk, t_own, t_dup, sel, pos_o, pos_d), off_own, hi_own, lo_own, off_dup, hi_dup, lo_dup)
        returned, d_tabs = lax.optimization_barrier((returned, d_tabs))
        return take_rows(returned, slot), d_tabs

    return jax.shard_map(device_body, mesh=mesh, in_specs=(tok_spec, row_spec, row_spec, tab_spec, full_spec, full_spec, full_spec, full_spec), out_specs=(row_spec, tab_spec), check_vma=False)
```

```python
import functools

import jax
import jax.numpy as jnp
from jax import lax
from jax.experimental import pallas as pl
from jax.experimental.pallas import tpu as pltpu
from jax.sharding import PartitionSpec as P

NORM_EPS = 1e-6
GELU_K = 0.7978845608028654
GELU_C = 0.044715
DEAD = 1 << 30
TILE = 512
HALF = 256
LAG = 1
SEG_TILE = 256
ROWS = 256
CHUNKS = 4
VMEM = 66_000_000
BF = jnp.bfloat16
F32 = jnp.float32


def dot(a, b):
    return lax.dot_general(a, b, (((1,), (0,)), ((), ())), preferred_element_type=F32)


def dot_t(a, b):
    return lax.dot_general(a, b, (((1,), (1,)), ((), ())), preferred_element_type=F32)


def gelu_both(p):
    sq = p * p
    half = 0.5 * jnp.tanh(p * (GELU_K + (GELU_K * GELU_C) * sq))
    cdf = 0.5 + half
    value = p * cdf
    slope = (0.5 - half) * (2.0 * GELU_K + (6.0 * GELU_K * GELU_C) * sq)
    return value, cdf + value * slope


def weave(streams):
    waiting = [LAG * k for k in range(len(streams))]
    alive = list(streams)
    while alive:
        for k, stream in enumerate(streams):
            if stream not in alive:
                continue
            if waiting[k] > 0:
                waiting[k] -= 1
            elif next(stream, None) is None:
                alive.remove(stream)


def fill_tiles(nt_ref, src, dst, sem, size):
    first, tile = pl.program_id(0) == 0, pl.program_id(1)

    def copy(t):
        rows = pl.ds(pl.multiple_of(t * size, size), size)
        return pltpu.make_async_copy(src.at[rows, :], dst.at[rows, :], sem.at[t])

    @pl.when(jnp.logical_and(first, tile == 0))
    def _():
        for t in range(src.shape[0] // size):
            pl.when(t < nt_ref[0])(copy(t).start)

    pl.when(first)(lambda: copy(tile).wait())


def forward_kernel(save, last, chained, nt_ref, *refs):
    pl.when(pl.program_id(1) < nt_ref[0])(lambda: forward_tile(save, last, chained, nt_ref, *refs))


def forward_tile(save, last, chained, nt_ref, n_ref, x_ref, e_ref, wu_ref, wd_ref, wg_ref, wp_ref, *rest):
    rest = list(rest)
    if chained:
        rest.pop(0)
    if save:
        xl_ref, du_ref, dg_ref = rest[:3]
        rest = rest[3:]
    a_ref = rest.pop(0)
    if last:
        out_ref = rest.pop(0)
    x_scr, sem = rest
    layer, tile = pl.program_id(0), pl.program_id(1)
    size = a_ref.shape[1]
    fill_tiles(nt_ref, x_ref, x_scr, sem, size)

    ff = wu_ref.shape[2]
    step = ff // CHUNKS
    cols = [slice(c * step, (c + 1) * step) for c in range(CHUNKS)]

    def stream(k, down):
        part = slice(k * HALF, (k + 1) * HALF)
        rows = pl.ds(pl.multiple_of(tile * size + k * HALF, HALF), HALF)
        x_bf = x_scr[rows, :]
        if save:
            xl_ref[0, part, :] = x_bf
        x = x_bf.astype(F32)
        r = lax.rsqrt(jnp.mean(x * x, axis=-1, keepdims=True) + NORM_EPS)
        u = (x * r).astype(BF)
        pre_gate = dot(u, wg_ref[0])
        now = dot(u, wu_ref[0, :, cols[0]])
        yield True
        gate, d_gate = gelu_both(pre_gate)
        a = gate.astype(BF)
        a_ref[0, part, :] = a
        if save:
            dg_ref[0, part, :] = d_gate
        acc = None
        for c in range(CHUNKS):
            if c + 1 < CHUNKS:
                later = dot(u, wu_ref[0, :, cols[c + 1]])
            h, d_up = gelu_both(now)
            if save:
                du_ref[0, part, cols[c]] = d_up
            if down:
                if c == 0:
                    s = (a.astype(F32) * e_ref[0, part, :].astype(F32)).astype(BF)
                    acc = x + dot(s, wp_ref[0])
                acc = acc + dot(h.astype(BF), wd_ref[0, cols[c], :])
            if c + 1 < CHUNKS:
                now = later
            yield True
        if down:
            x_new = acc.astype(BF)
            x_scr[rows, :] = x_new
            if last:
                out_ref[part, :] = x_new

    def run(down, parts):
        weave([stream(k, down) for k in range(parts)])

    both = n_ref[0] > tile * size + HALF
    full = jnp.bool_(True) if last else layer < pl.num_programs(0) - 1
    pl.when(jnp.logical_and(full, both))(lambda: run(True, 2))
    pl.when(jnp.logical_and(full, jnp.logical_not(both)))(lambda: run(True, 1))
    if not last:
        pl.when(jnp.logical_not(full))(lambda: run(False, 2))


def backward_kernel(nt_ref, n_ref, *refs):
    pl.when(pl.program_id(1) < nt_ref[0])(lambda: backward_tile(nt_ref, n_ref, *refs))


def backward_tile(nt_ref, n_ref, d_ref, xl_ref, du_ref, dg_ref, a_ref, e_ref, wu_ref, wd_ref, wg_ref, wp_ref, hi_ref, lo_ref, c_scr, sem):
    step_id, tile = pl.program_id(0), pl.program_id(1)
    size = xl_ref.shape[1]

    fill_tiles(nt_ref, d_ref, c_scr, sem, size)

    ff = wu_ref.shape[2]
    step = ff // CHUNKS
    cols = [slice(c * step, (c + 1) * step) for c in range(CHUNKS)]

    def stream(k, down):
        part = slice(k * HALF, (k + 1) * HALF)
        rows = pl.ds(pl.multiple_of(tile * size + k * HALF, HALF), HALF)
        c = c_scr[rows, :]
        ds = dot_t(c, wp_ref[0]).astype(BF)
        if down:
            now = dot_t(c, wd_ref[0, cols[0], :])
            later = dot_t(c, wd_ref[0, cols[1], :])
        yield True
        ds_f = ds.astype(F32)
        live = tile * size + k * HALF + lax.broadcasted_iota(jnp.int32, ds_f.shape, 0) < n_ref[0]
        grad = jnp.where(live, a_ref[0, part, :].astype(F32) * ds_f, 0.0)
        hi = grad.astype(BF)
        hi_ref[0, part, :] = hi
        lo_ref[0, part, :] = (grad - hi.astype(F32)).astype(BF)
        if down:
            de = (ds_f * e_ref[0, part, :].astype(F32)).astype(BF)
            dgate = (dg_ref[0, part, :] * de.astype(F32)).astype(BF)
            yield True
            m = dot_t(dgate, wg_ref[0])
            for q in range(CHUNKS):
                dup = (du_ref[0, part, cols[q]] * now.astype(BF).astype(F32)).astype(BF)
                now = later
                if q + 2 < CHUNKS:
                    later = dot_t(c, wd_ref[0, cols[q + 2], :])
                m = m + dot_t(dup, wu_ref[0, :, cols[q]])
                yield True
            x = xl_ref[0, part, :].astype(F32)
            r = lax.rsqrt(jnp.mean(x * x, axis=-1, keepdims=True) + NORM_EPS)
            n = x * r
            corr = jnp.mean(m * n, axis=-1, keepdims=True)
            c_scr[rows, :] = (c.astype(F32) + r * (m - n * corr)).astype(BF)

    def run(down, parts):
        weave([stream(k, down) for k in range(parts)])

    both = n_ref[0] > tile * size + HALF
    upper = step_id < pl.num_programs(0) - 1
    pl.when(jnp.logical_and(upper, both))(lambda: run(True, 2))
    pl.when(jnp.logical_and(upper, jnp.logical_not(both)))(lambda: run(True, 1))
    pl.when(jnp.logical_not(upper))(lambda: run(False, 2))


def run_forward(base, count, save, last, nt, live, x, e, w_up, w_down, w_gate, w_proj, a_prev=None):
    n, dim = x.shape
    layers, _, ff = w_up.shape
    t = TILE

    def per_layer(l, i, nt_ref, n_ref):
        return (l + base, 0, 0)

    def saved(l, i, nt_ref, n_ref):
        return (jnp.maximum(l + base - 1, 0), jnp.minimum(i, nt_ref[0] - 1), 0)

    def tok(l, i, nt_ref, n_ref):
        return (l + base, jnp.minimum(i, nt_ref[0] - 1), 0)

    outs = []
    if save:
        outs = [
            (jax.ShapeDtypeStruct((layers - 1, n, dim), BF), pl.BlockSpec((1, t, dim), saved)),
            (jax.ShapeDtypeStruct((layers - 1, n, ff), F32), pl.BlockSpec((1, t, ff), saved)),
            (jax.ShapeDtypeStruct((layers - 1, n, dim), F32), pl.BlockSpec((1, t, dim), saved)),
        ]
    outs.append((jax.ShapeDtypeStruct((layers, n, dim), BF), pl.BlockSpec((1, t, dim), tok)))
    aliases = {} if a_prev is None else {8: len(outs) - 1}
    if last:
        outs.append((jax.ShapeDtypeStruct((n, dim), BF), pl.BlockSpec((t, dim), lambda l, i, nt_ref, n_ref: (jnp.minimum(i, nt_ref[0] - 1), 0))))
    extra = [] if a_prev is None else [a_prev]
    flops = count * n * 2 * dim * (2 * ff + 2 * dim)
    return pl.pallas_call(
        functools.partial(forward_kernel, save, last, a_prev is not None),
        out_shape=[o[0] for o in outs],
        grid_spec=pltpu.PrefetchScalarGridSpec(
            num_scalar_prefetch=2, grid=(count, n // t),
            in_specs=[pl.BlockSpec(memory_space=pl.ANY), pl.BlockSpec((1, t, dim), tok),
                      pl.BlockSpec((1, dim, ff), per_layer), pl.BlockSpec((1, ff, dim), per_layer),
                      pl.BlockSpec((1, dim, dim), per_layer), pl.BlockSpec((1, dim, dim), per_layer)]
                     + [pl.BlockSpec(memory_space=pl.ANY)] * len(extra),
            out_specs=[o[1] for o in outs],
            scratch_shapes=[pltpu.VMEM((n, dim), BF), pltpu.SemaphoreType.DMA((n // t,))]),
        input_output_aliases=aliases,
        compiler_params=pltpu.CompilerParams(dimension_semantics=("arbitrary", "arbitrary"), vmem_limit_bytes=VMEM),
        cost_estimate=pl.CostEstimate(flops=flops // 2, bytes_accessed=n * ff * 4 * count, transcendentals=0),
        name="fwd",
    )(nt, live, x, e, w_up, w_down, w_gate, w_proj, *extra)


def run_backward(nt, n_live, d, xl, du, dg, a, e, w_up, w_down, w_gate, w_proj):
    n, dim = d.shape
    layers, _, ff = w_up.shape
    t = TILE
    top = layers - 1

    def per_layer(g, i, nt_ref, n_ref):
        return (top - g, 0, 0)

    def upper_layer(g, i, nt_ref, n_ref):
        return (jnp.maximum(top - g, 1), 0, 0)

    def saved(g, i, nt_ref, n_ref):
        return (jnp.maximum(top - 1 - g, 0), jnp.where(g == top, nt_ref[0] - 1, jnp.minimum(i, nt_ref[0] - 1)), 0)

    def tok(g, i, nt_ref, n_ref):
        return (top - g, jnp.minimum(i, nt_ref[0] - 1), 0)

    flops = layers * n * 2 * dim * (2 * ff + 2 * dim)
    return pl.pallas_call(
        backward_kernel,
        out_shape=[jax.ShapeDtypeStruct((layers, n, dim), BF)] * 2,
        grid_spec=pltpu.PrefetchScalarGridSpec(
            num_scalar_prefetch=2, grid=(layers, n // t),
            in_specs=[pl.BlockSpec(memory_space=pl.ANY), pl.BlockSpec((1, t, dim), saved),
                      pl.BlockSpec((1, t, ff), saved), pl.BlockSpec((1, t, dim), saved),
                      pl.BlockSpec((1, t, dim), tok), pl.BlockSpec((1, t, dim), tok),
                      pl.BlockSpec((1, dim, ff), upper_layer), pl.BlockSpec((1, ff, dim), upper_layer),
                      pl.BlockSpec((1, dim, dim), upper_layer), pl.BlockSpec((1, dim, dim), per_layer)],
            out_specs=[pl.BlockSpec((1, t, dim), tok)] * 2,
            scratch_shapes=[pltpu.VMEM((n, dim), BF), pltpu.SemaphoreType.DMA((n // t,))]),
        compiler_params=pltpu.CompilerParams(dimension_semantics=("arbitrary", "arbitrary"), vmem_limit_bytes=VMEM),
        cost_estimate=pl.CostEstimate(flops=flops // 2, bytes_accessed=n * ff * 4 * layers, transcendentals=0),
        name="bwd",
    )(nt, n_live, d, xl, du, dg, a, e, w_up, w_down, w_gate, w_proj)


def pick_kernel(rows_dev, num_ref, *refs):
    pl.when(pl.program_id(0) < num_ref[0])(lambda: pick_step(rows_dev, *refs))


def pick_step(rows_dev, tile_ref, blk_ref, pos, off_ref, tab_ref, e_ref):
    p = pl.program_id(0)
    blk, tile = blk_ref[p], tile_ref[p]
    layers, size = tab_ref.shape[0], tab_ref.shape[1]
    t, part = off_ref.shape[2], 128
    valid = rows_dev - blk * size
    tail = valid < size

    @pl.when(jnp.logical_or(p == 0, tile != tile_ref[jnp.maximum(p - 1, 0)]))
    def _():
        e_ref[...] = jnp.zeros_like(e_ref)

    def add(j, clip):
        cols = slice(j * part, (j + 1) * part)
        hot = (off_ref[0, :, cols] - blk * size == lax.broadcasted_iota(jnp.int32, (size, part), 0)).astype(F32)
        hot = hot.T.astype(BF)
        for l in range(layers):
            rows = tab_ref[l]
            if clip:
                keep = lax.broadcasted_iota(jnp.int32, rows.shape, 0) < valid
                rows = jnp.where(keep, rows.astype(F32), 0.0).astype(BF)
            e_ref[l, cols, :] += dot(hot, rows).astype(BF)

    for j in range(t // part):
        at = tile * t + j * part
        meets = jnp.logical_and(at < pos[blk + 1], at + part > pos[blk])
        pl.when(jnp.logical_and(meets, tail))(functools.partial(add, j, True))
        pl.when(jnp.logical_and(meets, jnp.logical_not(tail)))(functools.partial(add, j, False))


def run_pick(pairs, tile, blk, pos, off, tables):
    layers, rows_dev, dim = tables.shape
    n = off.shape[0]
    t = TILE
    return pl.pallas_call(
        functools.partial(pick_kernel, rows_dev),
        out_shape=jax.ShapeDtypeStruct((layers, n, dim), BF),
        grid_spec=pltpu.PrefetchScalarGridSpec(
            num_scalar_prefetch=4, grid=(tile.shape[0],),
            in_specs=[pl.BlockSpec((1, 1, t), lambda p, nr, tr, br, po: (tr[p], 0, 0)),
                      pl.BlockSpec((layers, ROWS, dim), lambda p, nr, tr, br, po: (0, br[p], 0))],
            out_specs=pl.BlockSpec((layers, t, dim), lambda p, nr, tr, br, po: (0, tr[p], 0))),
        compiler_params=pltpu.CompilerParams(dimension_semantics=("arbitrary",), vmem_limit_bytes=VMEM),
        cost_estimate=pl.CostEstimate(flops=40_000_000_000, bytes_accessed=n * dim * 16, transcendentals=0),
        name="pick",
    )(pairs.reshape(1), tile, blk, pos, off.reshape(n // t, 1, t), tables)


def sum_kernel(num_ref, *refs):
    pl.when(pl.program_id(0) < num_ref[0])(lambda: sum_step(*refs))


def sum_step(blk_ref, own_ref, dup_ref, sel_ref, pos_own, pos_dup, off_o, hi_o, lo_o, off_d, hi_d, lo_d, out_ref):
    s = pl.program_id(0)
    blk = blk_ref[s]
    layers, rows, dim = out_ref.shape
    t = off_o.shape[2]
    half = 128

    @pl.when(jnp.logical_or(s == 0, blk != blk_ref[jnp.maximum(s - 1, 0)]))
    def _():
        out_ref[...] = jnp.zeros_like(out_ref)

    def add(tile, pos, off_ref, hi_ref, lo_ref):
        first, end = pos[blk], pos[blk + 1]
        for j in range(t // half):
            at = tile * t + j * half

            @pl.when(jnp.logical_and(at < end, at + half > first))
            def _():
                cols = pl.ds(j * half, half)
                hot = (off_ref[0, :, cols] - blk * rows == lax.broadcasted_iota(jnp.int32, (rows, half), 0)).astype(F32).astype(BF)
                hot = jnp.concatenate([hot, hot], axis=1)
                for l in range(layers):
                    both = jnp.concatenate([hi_ref[l, cols, :], lo_ref[l, cols, :]], axis=0)
                    out_ref[l] += dot(hot, both)

    @pl.when(sel_ref[s] == 0)
    def _():
        add(own_ref[s], pos_own, off_o, hi_o, lo_o)

    @pl.when(sel_ref[s] == 1)
    def _():
        add(dup_ref[s], pos_dup, off_d, hi_d, lo_d)


def run_sum(rows_dev, steps, lists, off_own, hi_own, lo_own, off_dup, hi_dup, lo_dup):
    layers, n, dim = hi_own.shape
    t = SEG_TILE
    own = lambda s, m, b, o, d, se, po, pd: (0, o[s], 0)
    dup = lambda s, m, b, o, d, se, po, pd: (0, d[s], 0)
    own_off = lambda s, m, b, o, d, se, po, pd: (o[s], 0, 0)
    dup_off = lambda s, m, b, o, d, se, po, pd: (d[s], 0, 0)
    big = (layers, t, dim)
    return pl.pallas_call(
        sum_kernel,
        out_shape=jax.ShapeDtypeStruct((layers, rows_dev, dim), F32),
        grid_spec=pltpu.PrefetchScalarGridSpec(
            num_scalar_prefetch=7, grid=(lists[0].shape[0],),
            in_specs=[pl.BlockSpec((1, 1, t), own_off), pl.BlockSpec(big, own), pl.BlockSpec(big, own),
                      pl.BlockSpec((1, 1, t), dup_off), pl.BlockSpec(big, dup), pl.BlockSpec(big, dup)],
            out_specs=pl.BlockSpec((layers, ROWS, dim), lambda s, m, b, o, d, se, po, pd: (0, b[s], 0))),
        compiler_params=pltpu.CompilerParams(dimension_semantics=("arbitrary",), vmem_limit_bytes=VMEM),
        cost_estimate=pl.CostEstimate(flops=60_000_000_000, bytes_accessed=layers * dim * 4 * (2 * n + rows_dev), transcendentals=0),
        name="tabsum",
    )(steps.reshape(1), *lists, off_own.reshape(n // t, 1, t), hi_own, lo_own, off_dup.reshape(n // t, 1, t), hi_dup, lo_dup)


def spans(off, n_blocks, size):
    edges = jnp.arange(n_blocks + 1, dtype=jnp.int32) * ROWS
    pos = jnp.sum((off[None, :] < edges[:, None]).astype(jnp.int32), axis=1)
    return pos, *meeting(pos, size)


def meeting(pos, size):
    first = pos[:-1] // size
    return first, jnp.where(pos[1:] > pos[:-1], (pos[1:] - 1) // size - first + 1, 0)


def pick_at(one_hot, values):
    return jnp.sum(one_hot * values[None, :], axis=1)


def expand(count, length):
    end = jnp.cumsum(count)
    step = jnp.minimum(jnp.arange(length, dtype=jnp.int32), end[-1] - 1)
    begin = end - count
    in_block = jnp.logical_and(step[:, None] >= begin[None, :], step[:, None] < end[None, :]).astype(jnp.int32)
    return in_block, step - pick_at(in_block, begin), end[-1]


def take_rows(rows, idx):
    return rows.at[idx].get(mode='promise_in_bounds')


def solution(mesh):
    emb_size = mesh.shape['emb']
    dp_size = mesh.shape['dp']
    tok_spec = P(('dp', 'emb'))
    row_spec = P(('dp', 'emb'), None)
    tab_spec = P(None, 'emb', None)
    full_spec = P()

    def device_body(ids, x_loc, dy_loc, tabs, w_up, w_down, w_gate, w_proj):
        tok_dev = ids.shape[0]
        layers, rows_dev, dim = tabs.shape
        cap = 2 * tok_dev // emb_size
        n = emb_size * cap
        n_blocks = -(-rows_dev // ROWS)
        iota_tok = jnp.arange(tok_dev, dtype=jnp.int32)
        iota_n = jnp.arange(n, dtype=jnp.int32)

        ids_sorted, order = lax.sort((ids, iota_tok), num_keys=1)
        bounds = jnp.arange(emb_size + 1, dtype=jnp.int32) * rows_dev
        starts = jnp.sum((ids[None, :] < bounds[:, None]).astype(jnp.int32), axis=1)
        ids_pad = jnp.concatenate([ids_sorted, jnp.full((cap,), DEAD, jnp.int32)])
        order_pad = jnp.concatenate([order, jnp.zeros((cap,), jnp.int32)])
        slot_id = jnp.stack([lax.dynamic_slice(ids_pad, (starts[o],), (cap,)) for o in range(emb_size)])
        slot_src = jnp.concatenate([lax.dynamic_slice(order_pad, (starts[o],), (cap,)) for o in range(emb_size)])
        rank = jnp.arange(cap, dtype=jnp.int32)[None, :]
        alive = rank < (starts[1:] - starts[:-1])[:, None]
        send_off = jnp.where(alive, slot_id - bounds[:-1, None], DEAD)
        recv_off = lax.all_to_all(send_off, 'emb', 0, 0, tiled=True).reshape(n)

        def exchange(rows):
            return lax.all_to_all(rows.reshape(emb_size, cap, dim), 'emb', 0, 0, tiled=True).reshape(n, dim)

        off_own, order_own = lax.sort((recv_off, iota_n), num_keys=1)
        swap = [(i, dp_size - 1 - i) for i in range(dp_size)]
        off_dup = lax.ppermute(off_own, 'dp', swap)

        def lookup(off):
            live = jnp.sum((off < DEAD).astype(jnp.int32)).reshape(1)
            tiles = jnp.maximum((live + TILE - 1) // TILE, 1)
            pos, first, count = spans(off, n_blocks, TILE)
            hot, inner, pairs = expand(count, n // TILE + n_blocks)
            tile = jnp.clip(pick_at(hot, first) + inner, 0, n // TILE - 1)
            blk = pick_at(hot, jnp.arange(n_blocks, dtype=jnp.int32))
            return run_pick(pairs, tile, blk, pos, off, tabs), live, tiles, pos

        x_recv = exchange(take_rows(x_loc, slot_src))
        d_send = take_rows(dy_loc, slot_src)
        e_own, live_own, tiles_own, pos_o = lookup(off_own)
        e_dup, live_dup, tiles_dup, pos_d = lookup(off_dup)
        d_send, e_own, e_dup = lax.optimization_barrier((d_send, e_own, e_dup))
        x_recv, e_own, e_dup = lax.optimization_barrier((x_recv, e_own, e_dup))
        d_recv = exchange(d_send)
        weights = (w_up, w_down, w_gate, w_proj)
        x_own = take_rows(x_recv, order_own)
        x_dup = lax.ppermute(x_own, 'dp', swap)
        a_first, x_one = run_forward(0, 1, False, True, tiles_own, live_own, x_own, e_own, *weights)
        d_recv, x_one, a_first = lax.optimization_barrier((d_recv, x_one, a_first))
        d_own = take_rows(d_recv, order_own)
        d_dup = lax.ppermute(d_own, 'dp', swap)
        d_own, x_one, a_first = lax.optimization_barrier((d_own, x_one, a_first))
        xl, du, dg, a, x_fin = run_forward(1, layers - 1, True, True, tiles_own, live_own, x_one, e_own, *weights, a_prev=a_first)
        hi_own, lo_own = run_backward(tiles_own, live_own, d_own, xl, du, dg, a, e_own, *weights)
        x_dup, hi_own, lo_own = lax.optimization_barrier((x_dup, hi_own, lo_own))
        xl, du, dg, a = run_forward(0, layers, True, False, tiles_dup, live_dup, x_dup, e_dup, *weights)
        hi_dup, lo_dup = run_backward(tiles_dup, live_dup, d_dup, xl, du, dg, a, e_dup, *weights)

        _, back = lax.sort((order_own, iota_n), num_keys=1)
        _, place = lax.sort((order, iota_tok), num_keys=1)
        x_fin, hi_dup, lo_dup = lax.optimization_barrier((x_fin, hi_dup, lo_dup))
        returned = exchange(take_rows(x_fin, back))
        owner_hot = (ids[:, None] // rows_dev == jnp.arange(emb_size, dtype=jnp.int32)[None, :]).astype(jnp.int32)
        slot = place + pick_at(owner_hot, jnp.arange(emb_size, dtype=jnp.int32) * cap - starts[:-1])

        first_o, count_o = meeting(pos_o, SEG_TILE)
        first_d, count_d = meeting(pos_d, SEG_TILE)
        per_block = jnp.maximum(count_o + count_d, 1)
        hot, inner, steps = expand(per_block, 2 * (n // SEG_TILE + n_blocks))
        n_own = pick_at(hot, count_o)
        sel = (inner >= n_own).astype(jnp.int32)
        top = n // SEG_TILE - 1
        t_own = jnp.clip(pick_at(hot, first_o) + jnp.minimum(inner, jnp.maximum(n_own - 1, 0)), 0, top)
        t_dup = jnp.clip(pick_at(hot, first_d) + jnp.maximum(inner - n_own, 0), 0, top)
        blk = pick_at(hot, jnp.arange(n_blocks, dtype=jnp.int32))
        d_tabs = run_sum(rows_dev, steps, (blk, t_own, t_dup, sel, pos_o, pos_d), off_own, hi_own, lo_own, off_dup, hi_dup, lo_dup)
        returned, d_tabs = lax.optimization_barrier((returned, d_tabs))
        return take_rows(returned, slot), d_tabs

    return jax.shard_map(device_body, mesh=mesh, in_specs=(tok_spec, row_spec, row_spec, tab_spec, full_spec, full_spec, full_spec, full_spec), out_specs=(row_spec, tab_spec), check_vma=False)
```

```python
import functools

import jax
import jax.numpy as jnp
from jax import lax
from jax.experimental import pallas as pl
from jax.experimental.pallas import tpu as pltpu
from jax.sharding import PartitionSpec as P

NORM_EPS = 1e-6
GELU_K = 0.7978845608028654
GELU_C = 0.044715
DEAD = 1 << 30
TILE = 512
HALF = 256
LAG = 1
SEG_TILE = 256
ROWS = 256
CHUNKS = 4
VMEM = 66_000_000
BF = jnp.bfloat16
F32 = jnp.float32


def dot(a, b):
    return lax.dot_general(a, b, (((1,), (0,)), ((), ())), preferred_element_type=F32)


def dot_t(a, b):
    return lax.dot_general(a, b, (((1,), (1,)), ((), ())), preferred_element_type=F32)


def gelu_both(p):
    sq = p * p
    half = 0.5 * jnp.tanh(p * (GELU_K + (GELU_K * GELU_C) * sq))
    cdf = 0.5 + half
    value = p * cdf
    slope = (0.5 - half) * (2.0 * GELU_K + (6.0 * GELU_K * GELU_C) * sq)
    return value, cdf + value * slope


def weave(streams):
    waiting = [LAG * k for k in range(len(streams))]
    alive = list(streams)
    while alive:
        for k, stream in enumerate(streams):
            if stream not in alive:
                continue
            if waiting[k] > 0:
                waiting[k] -= 1
            elif next(stream, None) is None:
                alive.remove(stream)


def fill_tiles(nt_ref, src, dst, sem, size):
    first, tile = pl.program_id(0) == 0, pl.program_id(1)

    def copy(t):
        rows = pl.ds(pl.multiple_of(t * size, size), size)
        return pltpu.make_async_copy(src.at[rows, :], dst.at[rows, :], sem.at[t])

    @pl.when(jnp.logical_and(first, tile == 0))
    def _():
        for t in range(src.shape[0] // size):
            pl.when(t < nt_ref[0])(copy(t).start)

    pl.when(first)(lambda: copy(tile).wait())


def forward_kernel(save, last, chained, nt_ref, *refs):
    pl.when(pl.program_id(1) < nt_ref[0])(lambda: forward_tile(save, last, chained, nt_ref, *refs))


def forward_tile(save, last, chained, nt_ref, n_ref, x_ref, e_ref, wu_ref, wd_ref, wg_ref, wp_ref, *rest):
    rest = list(rest)
    if chained:
        rest.pop(0)
    if save:
        xl_ref, du_ref, dg_ref = rest[:3]
        rest = rest[3:]
    a_ref = rest.pop(0)
    if last:
        out_ref = rest.pop(0)
    x_scr, sem = rest
    layer, tile = pl.program_id(0), pl.program_id(1)
    size = a_ref.shape[1]
    fill_tiles(nt_ref, x_ref, x_scr, sem, size)

    ff = wu_ref.shape[2]
    step = ff // CHUNKS
    cols = [slice(c * step, (c + 1) * step) for c in range(CHUNKS)]

    def stream(k, down):
        part = slice(k * HALF, (k + 1) * HALF)
        rows = pl.ds(pl.multiple_of(tile * size + k * HALF, HALF), HALF)
        x_bf = x_scr[rows, :]
        if save:
            xl_ref[0, part, :] = x_bf
        x = x_bf.astype(F32)
        r = lax.rsqrt(jnp.mean(x * x, axis=-1, keepdims=True) + NORM_EPS)
        u = (x * r).astype(BF)
        pre_gate = dot(u, wg_ref[0])
        now = dot(u, wu_ref[0, :, cols[0]])
        yield True
        gate, d_gate = gelu_both(pre_gate)
        a = gate.astype(BF)
        a_ref[0, part, :] = a
        if save:
            dg_ref[0, part, :] = d_gate
        acc = None
        for c in range(CHUNKS):
            if c + 1 < CHUNKS:
                later = dot(u, wu_ref[0, :, cols[c + 1]])
            h, d_up = gelu_both(now)
            if save:
                du_ref[0, part, cols[c]] = d_up
            if down:
                if c == 0:
                    s = (a.astype(F32) * e_ref[0, part, :].astype(F32)).astype(BF)
                    acc = x + dot(s, wp_ref[0])
                acc = acc + dot(h.astype(BF), wd_ref[0, cols[c], :])
            if c + 1 < CHUNKS:
                now = later
            yield True
        if down:
            x_new = acc.astype(BF)
            x_scr[rows, :] = x_new
            if last:
                out_ref[part, :] = x_new

    def run(down, parts):
        weave([stream(k, down) for k in range(parts)])

    both = n_ref[0] > tile * size + HALF
    full = jnp.bool_(True) if last else layer < pl.num_programs(0) - 1
    pl.when(jnp.logical_and(full, both))(lambda: run(True, 2))
    pl.when(jnp.logical_and(full, jnp.logical_not(both)))(lambda: run(True, 1))
    if not last:
        pl.when(jnp.logical_not(full))(lambda: run(False, 2))


def backward_kernel(nt_ref, n_ref, *refs):
    pl.when(pl.program_id(1) < nt_ref[0])(lambda: backward_tile(nt_ref, n_ref, *refs))


def backward_tile(nt_ref, n_ref, d_ref, xl_ref, du_ref, dg_ref, a_ref, e_ref, wu_ref, wd_ref, wg_ref, wp_ref, hi_ref, lo_ref, c_scr, sem):
    step_id, tile = pl.program_id(0), pl.program_id(1)
    size = xl_ref.shape[1]

    fill_tiles(nt_ref, d_ref, c_scr, sem, size)

    ff = wu_ref.shape[2]
    step = ff // CHUNKS
    cols = [slice(c * step, (c + 1) * step) for c in range(CHUNKS)]

    def stream(k, down):
        part = slice(k * HALF, (k + 1) * HALF)
        rows = pl.ds(pl.multiple_of(tile * size + k * HALF, HALF), HALF)
        c = c_scr[rows, :]
        ds = dot_t(c, wp_ref[0]).astype(BF)
        if down:
            now = dot_t(c, wd_ref[0, cols[0], :])
            later = dot_t(c, wd_ref[0, cols[1], :])
        yield True
        ds_f = ds.astype(F32)
        live = tile * size + k * HALF + lax.broadcasted_iota(jnp.int32, ds_f.shape, 0) < n_ref[0]
        grad = jnp.where(live, a_ref[0, part, :].astype(F32) * ds_f, 0.0)
        hi = grad.astype(BF)
        hi_ref[0, part, :] = hi
        lo_ref[0, part, :] = (grad - hi.astype(F32)).astype(BF)
        if down:
            de = (ds_f * e_ref[0, part, :].astype(F32)).astype(BF)
            dgate = (dg_ref[0, part, :] * de.astype(F32)).astype(BF)
            yield True
            m = dot_t(dgate, wg_ref[0])
            for q in range(CHUNKS):
                dup = (du_ref[0, part, cols[q]] * now.astype(BF).astype(F32)).astype(BF)
                now = later
                if q + 2 < CHUNKS:
                    later = dot_t(c, wd_ref[0, cols[q + 2], :])
                m = m + dot_t(dup, wu_ref[0, :, cols[q]])
                yield True
            x = xl_ref[0, part, :].astype(F32)
            r = lax.rsqrt(jnp.mean(x * x, axis=-1, keepdims=True) + NORM_EPS)
            n = x * r
            corr = jnp.mean(m * n, axis=-1, keepdims=True)
            c_scr[rows, :] = (c.astype(F32) + r * (m - n * corr)).astype(BF)

    def run(down, parts):
        weave([stream(k, down) for k in range(parts)])

    both = n_ref[0] > tile * size + HALF
    upper = step_id < pl.num_programs(0) - 1
    pl.when(jnp.logical_and(upper, both))(lambda: run(True, 2))
    pl.when(jnp.logical_and(upper, jnp.logical_not(both)))(lambda: run(True, 1))
    pl.when(jnp.logical_not(upper))(lambda: run(False, 2))


def run_forward(base, count, save, last, nt, live, x, e, w_up, w_down, w_gate, w_proj, a_prev=None):
    n, dim = x.shape
    layers, _, ff = w_up.shape
    t = TILE

    def per_layer(l, i, nt_ref, n_ref):
        return (l + base, 0, 0)

    def saved(l, i, nt_ref, n_ref):
        return (jnp.maximum(l + base - 1, 0), jnp.minimum(i, nt_ref[0] - 1), 0)

    def tok(l, i, nt_ref, n_ref):
        return (l + base, jnp.minimum(i, nt_ref[0] - 1), 0)

    outs = []
    if save:
        outs = [
            (jax.ShapeDtypeStruct((layers - 1, n, dim), BF), pl.BlockSpec((1, t, dim), saved)),
            (jax.ShapeDtypeStruct((layers - 1, n, ff), F32), pl.BlockSpec((1, t, ff), saved)),
            (jax.ShapeDtypeStruct((layers - 1, n, dim), F32), pl.BlockSpec((1, t, dim), saved)),
        ]
    outs.append((jax.ShapeDtypeStruct((layers, n, dim), BF), pl.BlockSpec((1, t, dim), tok)))
    aliases = {} if a_prev is None else {8: len(outs) - 1}
    if last:
        outs.append((jax.ShapeDtypeStruct((n, dim), BF), pl.BlockSpec((t, dim), lambda l, i, nt_ref, n_ref: (jnp.minimum(i, nt_ref[0] - 1), 0))))
    extra = [] if a_prev is None else [a_prev]
    flops = count * n * 2 * dim * (2 * ff + 2 * dim)
    return pl.pallas_call(
        functools.partial(forward_kernel, save, last, a_prev is not None),
        out_shape=[o[0] for o in outs],
        grid_spec=pltpu.PrefetchScalarGridSpec(
            num_scalar_prefetch=2, grid=(count, n // t),
            in_specs=[pl.BlockSpec(memory_space=pl.ANY), pl.BlockSpec((1, t, dim), tok),
                      pl.BlockSpec((1, dim, ff), per_layer), pl.BlockSpec((1, ff, dim), per_layer),
                      pl.BlockSpec((1, dim, dim), per_layer), pl.BlockSpec((1, dim, dim), per_layer)]
                     + [pl.BlockSpec(memory_space=pl.ANY)] * len(extra),
            out_specs=[o[1] for o in outs],
            scratch_shapes=[pltpu.VMEM((n, dim), BF), pltpu.SemaphoreType.DMA((n // t,))]),
        input_output_aliases=aliases,
        compiler_params=pltpu.CompilerParams(dimension_semantics=("arbitrary", "arbitrary"), vmem_limit_bytes=VMEM),
        cost_estimate=pl.CostEstimate(flops=flops // 2, bytes_accessed=n * ff * 4 * count, transcendentals=0),
        name="fwd",
    )(nt, live, x, e, w_up, w_down, w_gate, w_proj, *extra)


def run_backward(nt, n_live, d, xl, du, dg, a, e, w_up, w_down, w_gate, w_proj):
    n, dim = d.shape
    layers, _, ff = w_up.shape
    t = TILE
    top = layers - 1

    def per_layer(g, i, nt_ref, n_ref):
        return (top - g, 0, 0)

    def upper_layer(g, i, nt_ref, n_ref):
        return (jnp.maximum(top - g, 1), 0, 0)

    def saved(g, i, nt_ref, n_ref):
        return (jnp.maximum(top - 1 - g, 0), jnp.where(g == top, nt_ref[0] - 1, jnp.minimum(i, nt_ref[0] - 1)), 0)

    def tok(g, i, nt_ref, n_ref):
        return (top - g, jnp.minimum(i, nt_ref[0] - 1), 0)

    flops = layers * n * 2 * dim * (2 * ff + 2 * dim)
    return pl.pallas_call(
        backward_kernel,
        out_shape=[jax.ShapeDtypeStruct((layers, n, dim), BF)] * 2,
        grid_spec=pltpu.PrefetchScalarGridSpec(
            num_scalar_prefetch=2, grid=(layers, n // t),
            in_specs=[pl.BlockSpec(memory_space=pl.ANY), pl.BlockSpec((1, t, dim), saved),
                      pl.BlockSpec((1, t, ff), saved), pl.BlockSpec((1, t, dim), saved),
                      pl.BlockSpec((1, t, dim), tok), pl.BlockSpec((1, t, dim), tok),
                      pl.BlockSpec((1, dim, ff), upper_layer), pl.BlockSpec((1, ff, dim), upper_layer),
                      pl.BlockSpec((1, dim, dim), upper_layer), pl.BlockSpec((1, dim, dim), per_layer)],
            out_specs=[pl.BlockSpec((1, t, dim), tok)] * 2,
            scratch_shapes=[pltpu.VMEM((n, dim), BF), pltpu.SemaphoreType.DMA((n // t,))]),
        compiler_params=pltpu.CompilerParams(dimension_semantics=("arbitrary", "arbitrary"), vmem_limit_bytes=VMEM),
        cost_estimate=pl.CostEstimate(flops=flops // 2, bytes_accessed=n * ff * 4 * layers, transcendentals=0),
        name="bwd",
    )(nt, n_live, d, xl, du, dg, a, e, w_up, w_down, w_gate, w_proj)


def pick_kernel(rows_dev, num_ref, *refs):
    pl.when(pl.program_id(0) < num_ref[0])(lambda: pick_step(rows_dev, *refs))


def pick_step(rows_dev, tile_ref, blk_ref, pos, off_ref, tab_ref, e_ref):
    p = pl.program_id(0)
    blk, tile = blk_ref[p], tile_ref[p]
    layers, size = tab_ref.shape[0], tab_ref.shape[1]
    t, part = off_ref.shape[2], 128
    valid = rows_dev - blk * size
    tail = valid < size

    @pl.when(jnp.logical_or(p == 0, tile != tile_ref[jnp.maximum(p - 1, 0)]))
    def _():
        e_ref[...] = jnp.zeros_like(e_ref)

    def add(j, clip):
        cols = slice(j * part, (j + 1) * part)
        hot = (off_ref[0, :, cols] - blk * size == lax.broadcasted_iota(jnp.int32, (size, part), 0)).astype(F32)
        hot = hot.T.astype(BF)
        for l in range(layers):
            rows = tab_ref[l]
            if clip:
                keep = lax.broadcasted_iota(jnp.int32, rows.shape, 0) < valid
                rows = jnp.where(keep, rows.astype(F32), 0.0).astype(BF)
            e_ref[l, cols, :] += dot(hot, rows).astype(BF)

    for j in range(t // part):
        at = tile * t + j * part
        meets = jnp.logical_and(at < pos[blk + 1], at + part > pos[blk])
        pl.when(jnp.logical_and(meets, tail))(functools.partial(add, j, True))
        pl.when(jnp.logical_and(meets, jnp.logical_not(tail)))(functools.partial(add, j, False))


def run_pick(pairs, tile, blk, pos, off, tables):
    layers, rows_dev, dim = tables.shape
    n = off.shape[0]
    t = TILE
    return pl.pallas_call(
        functools.partial(pick_kernel, rows_dev),
        out_shape=jax.ShapeDtypeStruct((layers, n, dim), BF),
        grid_spec=pltpu.PrefetchScalarGridSpec(
            num_scalar_prefetch=4, grid=(tile.shape[0],),
            in_specs=[pl.BlockSpec((1, 1, t), lambda p, nr, tr, br, po: (tr[p], 0, 0)),
                      pl.BlockSpec((layers, ROWS, dim), lambda p, nr, tr, br, po: (0, br[p], 0))],
            out_specs=pl.BlockSpec((layers, t, dim), lambda p, nr, tr, br, po: (0, tr[p], 0))),
        compiler_params=pltpu.CompilerParams(dimension_semantics=("arbitrary",), vmem_limit_bytes=VMEM),
        cost_estimate=pl.CostEstimate(flops=40_000_000_000, bytes_accessed=n * dim * 16, transcendentals=0),
        name="pick",
    )(pairs.reshape(1), tile, blk, pos, off.reshape(n // t, 1, t), tables)


def sum_kernel(num_ref, *refs):
    pl.when(pl.program_id(0) < num_ref[0])(lambda: sum_step(*refs))


def sum_step(blk_ref, own_ref, dup_ref, sel_ref, pos_own, pos_dup, off_o, hi_o, lo_o, off_d, hi_d, lo_d, out_ref):
    s = pl.program_id(0)
    blk = blk_ref[s]
    layers, rows, dim = out_ref.shape
    t = off_o.shape[2]
    half = 128

    @pl.when(jnp.logical_or(s == 0, blk != blk_ref[jnp.maximum(s - 1, 0)]))
    def _():
        out_ref[...] = jnp.zeros_like(out_ref)

    def add(tile, pos, off_ref, hi_ref, lo_ref):
        first, end = pos[blk], pos[blk + 1]
        for j in range(t // half):
            at = tile * t + j * half

            @pl.when(jnp.logical_and(at < end, at + half > first))
            def _():
                cols = pl.ds(j * half, half)
                hot = (off_ref[0, :, cols] - blk * rows == lax.broadcasted_iota(jnp.int32, (rows, half), 0)).astype(F32).astype(BF)
                hot = jnp.concatenate([hot, hot], axis=1)
                for l in range(layers):
                    both = jnp.concatenate([hi_ref[l, cols, :], lo_ref[l, cols, :]], axis=0)
                    out_ref[l] += dot(hot, both)

    @pl.when(sel_ref[s] == 0)
    def _():
        add(own_ref[s], pos_own, off_o, hi_o, lo_o)

    @pl.when(sel_ref[s] == 1)
    def _():
        add(dup_ref[s], pos_dup, off_d, hi_d, lo_d)


def run_sum(rows_dev, steps, lists, off_own, hi_own, lo_own, off_dup, hi_dup, lo_dup):
    layers, n, dim = hi_own.shape
    t = SEG_TILE
    own = lambda s, m, b, o, d, se, po, pd: (0, o[s], 0)
    dup = lambda s, m, b, o, d, se, po, pd: (0, d[s], 0)
    own_off = lambda s, m, b, o, d, se, po, pd: (o[s], 0, 0)
    dup_off = lambda s, m, b, o, d, se, po, pd: (d[s], 0, 0)
    big = (layers, t, dim)
    return pl.pallas_call(
        sum_kernel,
        out_shape=jax.ShapeDtypeStruct((layers, rows_dev, dim), F32),
        grid_spec=pltpu.PrefetchScalarGridSpec(
            num_scalar_prefetch=7, grid=(lists[0].shape[0],),
            in_specs=[pl.BlockSpec((1, 1, t), own_off), pl.BlockSpec(big, own), pl.BlockSpec(big, own),
                      pl.BlockSpec((1, 1, t), dup_off), pl.BlockSpec(big, dup), pl.BlockSpec(big, dup)],
            out_specs=pl.BlockSpec((layers, ROWS, dim), lambda s, m, b, o, d, se, po, pd: (0, b[s], 0))),
        compiler_params=pltpu.CompilerParams(dimension_semantics=("arbitrary",), vmem_limit_bytes=VMEM),
        cost_estimate=pl.CostEstimate(flops=60_000_000_000, bytes_accessed=layers * dim * 4 * (2 * n + rows_dev), transcendentals=0),
        name="tabsum",
    )(steps.reshape(1), *lists, off_own.reshape(n // t, 1, t), hi_own, lo_own, off_dup.reshape(n // t, 1, t), hi_dup, lo_dup)


def spans(off, n_blocks, size):
    edges = jnp.arange(n_blocks + 1, dtype=jnp.int32) * ROWS
    pos = jnp.sum((off[None, :] < edges[:, None]).astype(jnp.int32), axis=1)
    return pos, *meeting(pos, size)


def meeting(pos, size):
    first = pos[:-1] // size
    return first, jnp.where(pos[1:] > pos[:-1], (pos[1:] - 1) // size - first + 1, 0)


def pick_at(one_hot, values):
    return jnp.sum(one_hot * values[None, :], axis=1)


def expand(count, length):
    end = jnp.cumsum(count)
    step = jnp.minimum(jnp.arange(length, dtype=jnp.int32), end[-1] - 1)
    begin = end - count
    in_block = jnp.logical_and(step[:, None] >= begin[None, :], step[:, None] < end[None, :]).astype(jnp.int32)
    return in_block, step - pick_at(in_block, begin), end[-1]


def take_rows(rows, idx):
    return rows.at[idx].get(mode='promise_in_bounds')


def solution(mesh):
    emb_size = mesh.shape['emb']
    dp_size = mesh.shape['dp']
    tok_spec = P(('dp', 'emb'))
    row_spec = P(('dp', 'emb'), None)
    tab_spec = P(None, 'emb', None)
    full_spec = P()

    def device_body(ids, x_loc, dy_loc, tabs, w_up, w_down, w_gate, w_proj):
        tok_dev = ids.shape[0]
        layers, rows_dev, dim = tabs.shape
        cap = 2 * tok_dev // emb_size
        n = emb_size * cap
        n_blocks = -(-rows_dev // ROWS)
        iota_tok = jnp.arange(tok_dev, dtype=jnp.int32)
        iota_n = jnp.arange(n, dtype=jnp.int32)

        ids_sorted, order = lax.sort((ids, iota_tok), num_keys=1)
        bounds = jnp.arange(emb_size + 1, dtype=jnp.int32) * rows_dev
        starts = jnp.sum((ids[None, :] < bounds[:, None]).astype(jnp.int32), axis=1)
        ids_pad = jnp.concatenate([ids_sorted, jnp.full((cap,), DEAD, jnp.int32)])
        order_pad = jnp.concatenate([order, jnp.zeros((cap,), jnp.int32)])
        slot_id = jnp.stack([lax.dynamic_slice(ids_pad, (starts[o],), (cap,)) for o in range(emb_size)])
        slot_src = jnp.concatenate([lax.dynamic_slice(order_pad, (starts[o],), (cap,)) for o in range(emb_size)])
        rank = jnp.arange(cap, dtype=jnp.int32)[None, :]
        alive = rank < (starts[1:] - starts[:-1])[:, None]
        send_off = jnp.where(alive, slot_id - bounds[:-1, None], DEAD)
        recv_off = lax.all_to_all(send_off, 'emb', 0, 0, tiled=True).reshape(n)

        def exchange(rows):
            return lax.all_to_all(rows.reshape(emb_size, cap, dim), 'emb', 0, 0, tiled=True).reshape(n, dim)

        off_own, order_own = lax.sort((recv_off, iota_n), num_keys=1)
        swap = [(i, dp_size - 1 - i) for i in range(dp_size)]
        off_dup = lax.ppermute(off_own, 'dp', swap)

        def lookup(off):
            live = jnp.sum((off < DEAD).astype(jnp.int32)).reshape(1)
            tiles = jnp.maximum((live + TILE - 1) // TILE, 1)
            pos, first, count = spans(off, n_blocks, TILE)
            hot, inner, pairs = expand(count, n // TILE + n_blocks)
            tile = jnp.clip(pick_at(hot, first) + inner, 0, n // TILE - 1)
            blk = pick_at(hot, jnp.arange(n_blocks, dtype=jnp.int32))
            return run_pick(pairs, tile, blk, pos, off, tabs), live, tiles, pos

        x_recv = exchange(take_rows(x_loc, slot_src))
        d_send = take_rows(dy_loc, slot_src)
        e_own, live_own, tiles_own, pos_o = lookup(off_own)
        _, back = lax.sort((order_own, iota_n), num_keys=1)
        d_send, e_own, back = lax.optimization_barrier((d_send, e_own, back))
        x_recv, e_own = lax.optimization_barrier((x_recv, e_own))
        d_recv = exchange(d_send)
        weights = (w_up, w_down, w_gate, w_proj)
        x_own = take_rows(x_recv, order_own)
        x_dup = lax.ppermute(x_own, 'dp', swap)
        off_dup, x_own = lax.optimization_barrier((off_dup, x_own))
        e_dup, live_dup, tiles_dup, pos_d = lookup(off_dup)
        a_first, x_one = run_forward(0, 1, False, True, tiles_own, live_own, x_own, e_own, *weights)
        d_recv, x_one, a_first, e_dup = lax.optimization_barrier((d_recv, x_one, a_first, e_dup))
        d_own = take_rows(d_recv, order_own)
        d_dup = lax.ppermute(d_own, 'dp', swap)
        d_own, x_one, a_first = lax.optimization_barrier((d_own, x_one, a_first))
        xl, du, dg, a, x_fin = run_forward(1, layers - 1, True, True, tiles_own, live_own, x_one, e_own, *weights, a_prev=a_first)
        hi_own, lo_own = run_backward(tiles_own, live_own, d_own, xl, du, dg, a, e_own, *weights)
        x_dup, hi_own, lo_own = lax.optimization_barrier((x_dup, hi_own, lo_own))
        xl, du, dg, a = run_forward(0, layers, True, False, tiles_dup, live_dup, x_dup, e_dup, *weights)
        hi_dup, lo_dup = run_backward(tiles_dup, live_dup, d_dup, xl, du, dg, a, e_dup, *weights)

        _, place = lax.sort((order, iota_tok), num_keys=1)
        x_fin, hi_dup, lo_dup = lax.optimization_barrier((x_fin, hi_dup, lo_dup))
        returned = exchange(take_rows(x_fin, back))
        owner_hot = (ids[:, None] // rows_dev == jnp.arange(emb_size, dtype=jnp.int32)[None, :]).astype(jnp.int32)
        slot = place + pick_at(owner_hot, jnp.arange(emb_size, dtype=jnp.int32) * cap - starts[:-1])

        first_o, count_o = meeting(pos_o, SEG_TILE)
        first_d, count_d = meeting(pos_d, SEG_TILE)
        per_block = jnp.maximum(count_o + count_d, 1)
        hot, inner, steps = expand(per_block, 2 * (n // SEG_TILE + n_blocks))
        n_own = pick_at(hot, count_o)
        sel = (inner >= n_own).astype(jnp.int32)
        top = n // SEG_TILE - 1
        t_own = jnp.clip(pick_at(hot, first_o) + jnp.minimum(inner, jnp.maximum(n_own - 1, 0)), 0, top)
        t_dup = jnp.clip(pick_at(hot, first_d) + jnp.maximum(inner - n_own, 0), 0, top)
        blk = pick_at(hot, jnp.arange(n_blocks, dtype=jnp.int32))
        d_tabs = run_sum(rows_dev, steps, (blk, t_own, t_dup, sel, pos_o, pos_d), off_own, hi_own, lo_own, off_dup, hi_dup, lo_dup)
        returned, d_tabs = lax.optimization_barrier((returned, d_tabs))
        return take_rows(returned, slot), d_tabs

    return jax.shard_map(device_body, mesh=mesh, in_specs=(tok_spec, row_spec, row_spec, tab_spec, full_spec, full_spec, full_spec, full_spec), out_specs=(row_spec, tab_spec), check_vma=False)
```
